256 devices in a mesh: dp: 8 (over x, core), expert: 32 (over z, y).
Axes of the slice: x: 4, y: 4, z: 8, core: 2. Of those that a mesh axis runs over, the one named last changes fastest.
Arguments:
- tokens: bfloat16 [32768, 1024], P(('dp', 'expert')), may hold values from -6 to 6
- route_a: int32 [32768, 1], P(('dp', 'expert')), may hold values from 0 to 31
- route_b: int32 [32768, 1], P(('dp', 'expert')), may hold values from 0 to 63
- gain_a: float32 [1024], replicated, may hold values from 0.25 to 1.75
- gain_b: float32 [1024], replicated, may hold values from 0.25 to 1.75
- router_a: bfloat16 [1024, 32], replicated, may hold values from -0.375 to 0.375
- router_b: bfloat16 [1024, 64], replicated, may hold values from -0.375 to 0.375
- dense_in_a: bfloat16 [1024, 4096], P(None, 'dp'), may hold values from -0.1875 to 0.1875
- dense_out_a: bfloat16 [4096, 1024], P('dp'), may hold values from -0.09375 to 0.09375
- dense_in_b: bfloat16 [1024, 4096], P(None, 'dp'), may hold values from -0.1875 to 0.1875
- dense_out_b: bfloat16 [4096, 1024], P('dp'), may hold values from -0.09375 to 0.09375
- expert_in_a: bfloat16 [32, 1024, 4096], P('expert', None, 'dp'), may hold values from -0.1875 to 0.1875
- expert_out_a: bfloat16 [32, 4096, 1024], P('expert', 'dp'), may hold values from -0.09375 to 0.09375
- expert_in_b: bfloat16 [64, 1024, 4096], P('expert', None, 'dp'), may hold values from -0.1875 to 0.1875
- expert_out_b: bfloat16 [64, 4096, 1024], P('expert', 'dp'), may hold values from -0.09375 to 0.09375
Outputs:
- stream_out: bfloat16 [32768, 1024], P(('dp', 'expert'))
The draws below stay inside these ranges and needn't reach their ends.
All inputs are finite; a program needn't handle non-finite values.
Results may differ from the reference program's by a relative error of at most 0.0091.
Values may be sent and summed in bfloat16 or wider, within the bound.
A program may use at most 128 MiB of HBM per device.

```python
import jax
import jax.numpy as jnp
from jax import lax

D = 1024
FF = 4096
TOK_DEV = 128
EXPERTS_A = 32
EXPERTS_B = 64
TOKENS = 32768


def levels(own_key, dims, split, low, high):
    def one(dim, shards_of):
        heights = jax.random.uniform(jax.random.fold_in(jax.random.fold_in(own_key, 6), dim), (shards_of,), jnp.float32, low / len(split), high / len(split))
        return jnp.repeat(jnp.exp(heights), dims[dim] // shards_of).reshape((-1,) + (1,) * (len(dims) - dim - 1))

    loudness = one(*split[0])
    for cut in split[1:]:
        loudness = loudness * one(*cut)
    return loudness


def different_ones(stream_key, rows, amount, top, lift):
    order = jax.random.permutation(jax.random.fold_in(stream_key, 1), amount)
    pull = order
    for power in range(3):
        pull = pull * pull // amount
    pull = pull * lift // amount
    lots = jax.random.randint(jax.random.fold_in(stream_key, 2), (rows, amount), 0, 4096) + pull
    holders = jax.random.permutation(jax.random.fold_in(stream_key, 3), rows)[jnp.arange(amount) % rows]
    lots = jnp.where(jnp.arange(rows)[:, None] == holders[None, :], 1 << 14, lots)
    merit = lots * amount + jnp.arange(amount)
    return lax.top_k(merit.astype(jnp.int32), top)[1].astype(jnp.int32)


def gaussian(key, extent, deviation, limit, cuts=(), dtype=jnp.bfloat16):
    loudness = levels(key, extent, cuts, -0.22, 0.18) if cuts else 1.0
    array = jax.random.normal(key, extent, jnp.float32) * deviation * loudness
    return jnp.minimum(jnp.maximum(array, -limit), limit).astype(dtype)


def setup_inputs(seed: int = 0) -> dict:
    key_of = jax.random.split(jax.random.key(seed), 16)
    tokens = gaussian(key_of[0], (TOKENS, D), 1.0, 6.0, ((0, 256),))
    route_a = different_ones(key_of[1], TOKENS, EXPERTS_A, 1, 256)
    route_b = different_ones(key_of[2], TOKENS, EXPERTS_B, 1, 128)
    gain_a = jnp.clip(1.0 + 0.15 * jax.random.normal(key_of[3], (D,), jnp.float32), 0.25, 1.75)
    gain_b = jnp.clip(1.0 + 0.15 * jax.random.normal(key_of[4], (D,), jnp.float32), 0.25, 1.75)
    router_a = gaussian(key_of[5], (D, EXPERTS_A), (D // 4) ** -0.5, 0.375)
    router_b = gaussian(key_of[6], (D, EXPERTS_B), (D // 4) ** -0.5, 0.375)
    dense_in_a = gaussian(key_of[7], (D, FF), D ** -0.5, 0.1875, ((1, 8),))
    dense_out_a = gaussian(key_of[8], (FF, D), FF ** -0.5, 0.09375, ((0, 8),))
    dense_in_b = gaussian(key_of[9], (D, FF), D ** -0.5, 0.1875, ((1, 8),))
    dense_out_b = gaussian(key_of[10], (FF, D), FF ** -0.5, 0.09375, ((0, 8),))
    expert_in_a = gaussian(key_of[11], (EXPERTS_A, D, FF), D ** -0.5, 0.1875, ((0, 32), (2, 8)))
    expert_out_a = gaussian(key_of[12], (EXPERTS_A, FF, D), FF ** -0.5, 0.09375, ((0, 32), (1, 8)))
    expert_in_b = gaussian(key_of[13], (EXPERTS_B, D, FF), D ** -0.5, 0.1875, ((0, 32), (2, 8)))
    expert_out_b = gaussian(key_of[14], (EXPERTS_B, FF, D), FF ** -0.5, 0.09375, ((0, 32), (1, 8)))
    return dict(tokens=tokens, route_a=route_a, route_b=route_b, gain_a=gain_a, gain_b=gain_b, router_a=router_a, router_b=router_b, dense_in_a=dense_in_a, dense_out_a=dense_out_a, dense_in_b=dense_in_b, dense_out_b=dense_out_b, expert_in_a=expert_in_a, expert_out_a=expert_out_a, expert_in_b=expert_in_b, expert_out_b=expert_out_b)


def norm_rows(x, gain):
    xf = x.astype(jnp.float32)
    mean = lax.optimization_barrier(jnp.mean(xf, axis=-1, keepdims=True))
    var = lax.optimization_barrier(jnp.mean((xf - mean) ** 2, axis=-1, keepdims=True))
    return ((xf - mean) / jnp.sqrt(var + 1e-05) * gain).astype(jnp.bfloat16)

def moe_layer(x, ids, gain, router, d_in, d_out, e_in, e_out):
    experts = router.shape[1]
    devices = x.shape[0] // TOK_DEV
    cap = (5 * TOK_DEV + 4 * experts - 1) // (4 * experts)
    normed = norm_rows(x, gain)
    blocks = ids.reshape(devices, TOK_DEV).astype(jnp.int32)
    onehot = (blocks[:, :, None] == jnp.arange(experts).astype(jnp.int32)[None, None, :]).astype(jnp.int32)
    before = (jnp.cumsum(onehot, axis=1) - onehot).astype(jnp.int32)
    rank = lax.optimization_barrier(jnp.sum(before * onehot, axis=-1)).astype(jnp.int32)
    kept = rank < cap
    total = devices * experts * cap
    anchor = jnp.arange(devices).astype(jnp.int32)[:, None] * (experts * cap)
    flat = jnp.where(kept, anchor + blocks * cap + rank, total).reshape(-1).astype(jnp.int32)
    logits = jnp.dot(normed, router, preferred_element_type=jnp.float32)
    picked = lax.optimization_barrier(jnp.sum(logits * onehot.reshape(-1, experts).astype(jnp.float32), axis=-1))
    gate = jax.nn.sigmoid(picked) * kept.reshape(-1).astype(jnp.float32)
    buffer = jnp.zeros((total, normed.shape[1]), jnp.bfloat16).at[flat].set(normed, mode='drop')
    buffer = buffer.reshape(devices, experts, cap, -1).transpose(1, 0, 2, 3).reshape(experts, devices * cap, -1)

    def one_expert(args):
        rows, w_first, w_second = args
        act = jax.nn.gelu(jnp.dot(rows, w_first, preferred_element_type=jnp.float32), approximate=True).astype(jnp.bfloat16)
        return jnp.dot(act, w_second, preferred_element_type=jnp.float32)
    outputs = lax.map(one_expert, (buffer, e_in, e_out))
    outputs = outputs.reshape(experts, devices, cap, -1).transpose(1, 0, 2, 3).reshape(total, -1)
    expert_tok = jnp.take(outputs, flat, axis=0, mode='fill', fill_value=0.0)

    def one_block(rows):
        act = jax.nn.gelu(jnp.dot(rows, d_in, preferred_element_type=jnp.float32), approximate=True).astype(jnp.bfloat16)
        return jnp.dot(act, d_out, preferred_element_type=jnp.float32)
    dense = lax.map(one_block, normed.reshape(devices, TOK_DEV, -1)).reshape(x.shape[0], -1)
    return (x.astype(jnp.float32) + dense + gate[:, None] * expert_tok).astype(jnp.bfloat16)

def reference(tokens, route_a, route_b, gain_a, gain_b, router_a, router_b, dense_in_a, dense_out_a, dense_in_b, dense_out_b, expert_in_a, expert_out_a, expert_in_b, expert_out_b):
    middle = moe_layer(tokens, route_a[:, 0], gain_a, router_a, dense_in_a, dense_out_a, expert_in_a, expert_out_a)
    return moe_layer(middle, route_b[:, 0], gain_b, router_b, dense_in_b, dense_out_b, expert_in_b, expert_out_b)
```

```python
import functools

import jax
import jax.numpy as jnp
from jax import lax
from jax.experimental import pallas as pl
from jax.experimental.pallas import tpu as pltpu
from jax.sharding import PartitionSpec as P

MESH = pl.DeviceIdType.MESH
BF = jnp.bfloat16
F32 = jnp.float32
PAD = 8


def dot(a, b):
    return jnp.dot(a, b, preferred_element_type=F32)


def ffn(rows, w_in, w_out):
    return dot(jax.nn.gelu(dot(rows, w_in), approximate=True).astype(BF), w_out)


class Place:
    def __init__(self, n_dp, n_ex):
        self.n_ex = n_ex
        chips = n_dp // 2
        self.d = lax.axis_index("dp")
        self.e = lax.axis_index("expert")
        x, c = self.d // 2, self.d % 2
        right = (lax.rem(x + 1, chips) * 2 + c, self.e)
        left = (lax.rem(x + chips - 1, chips) * 2 + c, self.e)
        self.along = (right, left)
        self.partner = (x * 2 + 1 - c, self.e)

    def ahead(self, o):
        return (self.d, lax.rem(self.e + o, self.n_ex))

    def behind(self, o):
        return (self.d, lax.rem(self.e + self.n_ex - o, self.n_ex))


class Ring:
    def __init__(self, place, blocks, partial, kept, sums, landed, sems):
        self.p = place
        self.g = blocks
        self.y1 = partial
        self.y0 = kept
        self.s = sums
        self.z = landed[0]
        self.f = landed[1]
        self.link_send, self.link_recv, self.core_send, self.core_recv = sems
        self.started = []

    def copy(self, src, dst, kind, slot, to):
        send, recv = (self.link_send, self.link_recv) if kind else (self.core_send, self.core_recv)
        return pltpu.make_async_remote_copy(
            src_ref=src,
            dst_ref=dst,
            send_sem=send.at[slot],
            recv_sem=recv.at[slot],
            device_id=to,
            device_id_type=MESH,
        )

    def start(self, make):
        made = make
        made.start()
        self.started.append(made)

    def gather_copy(self, u, h):
        if u == 1:
            return self.copy(self.g.at[0, h, 0], self.g.at[1, h, 0], 1, h, self.p.along[h])
        if u == 2:
            return self.copy(self.g.at[0, h, 0], self.g.at[2, h, 0], 1, 2 + h, self.p.along[1 - h])
        return self.copy(self.g.at[1, h, 0], self.g.at[3, h, 0], 1, 4 + h, self.p.along[h])

    def core_copy(self, u, h):
        return self.copy(self.g.at[u, h, 0], self.g.at[u, h, 1], 0, 2 * u + h, self.p.partner)

    def gather_start(self):
        for u in (1, 2):
            for h in (0, 1):
                self.start(self.gather_copy(u, h))
        for h in (0, 1):
            self.start(self.core_copy(0, h))

    def arrive(self, u):
        for h in (0, 1):
            self.gather_copy(u, h).wait_recv()
            if u == 1:
                self.start(self.gather_copy(3, h))
            self.start(self.core_copy(u, h))

    def compute(self, u, fn):
        for h in (0, 1):
            self.core_copy(u, h).wait_recv()
        fn(u)
        for h in (0, 1):
            self.start(self.sum_copy(u, h))

    def sum_copy(self, u, h):
        return self.copy(self.y1.at[u, h], self.z.at[u, h], 0, 8 + 2 * u + h, self.p.partner)

    def core_sum(self, u, h):
        self.sum_copy(u, h).wait_recv()
        return self.y0[u, h] + self.z[u, h].astype(F32)

    def scatter_copy(self, u, h):
        to = self.p.along[1 - h] if u == 1 else self.p.along[h]
        slot = {1: 0, 3: 1, 2: 2}[u]
        return self.copy(self.s.at[slot, h], self.f.at[slot, h], 1, 6 + 2 * slot + h, to)

    def scatter_near(self):
        for h in (0, 1):
            self.s[0, h] = self.core_sum(1, h).astype(BF)
            self.start(self.scatter_copy(1, h))

    def scatter_far(self):
        for h in (0, 1):
            self.s[1, h] = self.core_sum(3, h).astype(BF)
            self.start(self.scatter_copy(3, h))

    def scatter_last(self):
        for h in (0, 1):
            mine = self.core_sum(2, h)
            self.scatter_copy(3, h).wait_recv()
            self.s[2, h] = (mine + self.f[1, h].astype(F32)).astype(BF)
            self.start(self.scatter_copy(2, h))

    def total(self, h):
        mine = self.core_sum(0, h)
        self.scatter_copy(1, h).wait_recv()
        mine = mine + self.f[0, h].astype(F32)
        self.scatter_copy(2, h).wait_recv()
        return mine + self.f[2, h].astype(F32)

    def drain(self):
        for made in self.started:
            made.wait_send()


class Exchange:
    def __init__(self, place, out, into, send, recv, forward):
        self.p, self.out, self.into, self.send, self.recv = place, out, into, send, recv
        self.forward = forward

    def copy(self, o):
        return pltpu.make_async_remote_copy(
            src_ref=self.out.at[o],
            dst_ref=self.into.at[o],
            send_sem=self.send.at[o],
            recv_sem=self.recv.at[o],
            device_id=self.p.ahead(o) if self.forward else self.p.behind(o),
            device_id_type=MESH,
        )

    def start(self):
        def one(o, carry):
            self.copy(o).start()
            return carry

        lax.fori_loop(1, self.p.n_ex, one, 0)

    def arrived(self):
        def one(o, carry):
            self.copy(o).wait_recv()
            return carry

        lax.fori_loop(1, self.p.n_ex, one, 0)

    def drain(self):
        def one(o, carry):
            self.copy(o).wait_send()
            return carry

        lax.fori_loop(1, self.p.n_ex, one, 0)


def norm_rows(xf, gain):
    mean = jnp.mean(xf, axis=-1, keepdims=True)
    var = jnp.mean((xf - mean) ** 2, axis=-1, keepdims=True)
    return ((xf - mean) / jnp.sqrt(var + 1e-05) * gain).astype(BF)


def iota(shape, dim):
    return lax.broadcasted_iota(jnp.int32, shape, dim)


def routing(ids, place, experts, cap):
    tok = ids.shape[0]
    per_dev = experts // place.n_ex
    onehot = (ids == iota((tok, experts), 1)).astype(F32)
    below = (iota((tok, tok), 1) < iota((tok, tok), 0)).astype(F32)
    before = dot(below.astype(BF), onehot.astype(BF))
    rank = jnp.sum(before * onehot, axis=-1, keepdims=True)
    kept = rank < cap
    owner, inner = ids // per_dev, ids % per_dev
    offset = lax.rem(owner - place.e + place.n_ex, place.n_ex)
    row = (offset * PAD + inner * cap).astype(F32) + rank
    rows = place.n_ex * PAD
    spot = jnp.where(kept & (iota((tok, rows), 1).astype(F32) == row), 1.0, 0.0)
    return onehot, kept, spot


def packed_row(p, place, per_dev, cap):
    source, inner = p // PAD, p % PAD
    row = inner
    which = jnp.zeros_like(p)
    for k in range(1, per_dev):
        which = which + (inner >= k * cap).astype(jnp.int32)
    row = inner - which * cap
    return jnp.where(
        inner < per_dev * cap, which * (place.n_ex * cap) + source * cap + row, -1
    )


def kernel(
    n_dp,
    n_ex,
    *refs,
):
    (tokens, route_a, route_b, gain_a, gain_b, router_a, router_b) = refs[:7]
    weights = refs[7:15]
    out = refs[15]
    local = refs[16:24]
    weight_sem = refs[24]
    scratch = refs[25:]
    place = Place(n_dp, n_ex)
    loads = [
        pltpu.make_async_copy(weights[i], local[i], weight_sem.at[i]) for i in range(8)
    ]
    barrier = pltpu.get_barrier_semaphore()

    def greet(o, carry):
        pl.semaphore_signal(barrier, inc=1, device_id=place.ahead(o), device_id_type=MESH)
        return carry

    for to in (*place.along, place.partner):
        pl.semaphore_signal(barrier, inc=1, device_id=to, device_id_type=MESH)
    lax.fori_loop(1, n_ex, greet, 0)
    for i in (0, 1, 4, 5, 2, 3, 6, 7):
        loads[i].start()

    kept_dense, kept_expert = scratch[:2]
    per_layer = (len(scratch) - 2) // 2
    drains = []
    x = tokens[...].astype(F32)
    for layer in range(2):
        s = scratch[2 + layer * per_layer : 2 + (layer + 1) * per_layer]
        dense = Ring(place, s[0], s[1], kept_dense, s[2], s[3:5], s[5:9])
        s = s[9:]
        rows = s[0].shape[3]
        y0 = kept_expert.at[:, :, pl.ds(0, rows)]
        expert = Ring(place, s[0], s[1], y0, s[2], s[3:5], s[5:9])
        s = s[9:]
        go = Exchange(place, s[0], s[1], s[2], s[3], True)
        back = Exchange(place, s[4], s[5], s[6], s[7], False)
        drains += [dense, expert, go, back]
        ids = (route_a, route_b)[layer][...]
        router = (router_a, router_b)[layer][...]
        experts = router.shape[1]
        tok, width = tokens.shape
        per_dev = experts // n_ex
        cap = (5 * tok + 4 * experts - 1) // (4 * experts)
        d_in, d_out = local[4 * layer], local[4 * layer + 1]
        e_in, e_out = local[4 * layer + 2], local[4 * layer + 3]
        half = tok // 2

        normed = norm_rows(x, (gain_a, gain_b)[layer][...])
        for h in (0, 1):
            dense.g[0, h, 0] = normed[h * half : (h + 1) * half]
        onehot, kept, spot = routing(ids, place, experts, cap)
        if layer == 0:
            pl.semaphore_wait(barrier, n_ex - 1 + 3)
        dense.gather_start()
        messages = dot(spot.T.astype(BF), normed).astype(BF).reshape(n_ex, PAD, width)
        go.out[...] = messages
        go.into[0] = messages[0]
        go.start()
        logits = dot(normed, router)
        picked = jnp.sum(logits * onehot, axis=-1, keepdims=True)
        gate = jax.nn.sigmoid(picked) * kept.astype(F32)

        def dense_unit(u):
            y = ffn(dense.g[u].reshape(4 * half, width), d_in[...], d_out[...])
            y = y.reshape(2, 2, half, width)
            dense.y1[u] = y[:, 1].astype(BF)
            dense.y0[u] = y[:, 0]

        def expert_unit(u):
            if per_dev == 1:
                y = ffn(expert.g[u].reshape(4 * rows, width), e_in[0], e_out[0])
                y = y.reshape(2, 2, rows, width)
                expert.y1[u] = y[:, 1].astype(BF)
                expert.y0[u] = y[:, 0]
            else:
                for h in (0, 1):
                    y = ffn(expert.g[u, h].reshape(2 * rows, width), e_in[h], e_out[h])
                    y = y.reshape(2, rows, width)
                    expert.y1[u, h] = y[1].astype(BF)
                    expert.y0[u, h] = y[0]

        for i in (0, 1):
            loads[4 * layer + i].wait()
        dense.compute(0, dense_unit)
        dense.arrive(1)
        dense.compute(1, dense_unit)
        dense.arrive(2)

        go.arrived()
        slots = n_ex * PAD
        message = iota((2 * rows, slots), 1)
        pack = packed_row(message, place, per_dev, cap) == iota((2 * rows, slots), 0)
        block = dot(
            jnp.where(pack, 1.0, 0.0).astype(BF), go.into[...].reshape(slots, width)
        ).astype(BF)
        for h in (0, 1):
            expert.g[0, h, 0] = block[h * rows : (h + 1) * rows]
        expert.gather_start()
        dense.compute(2, dense_unit)
        dense.arrive(3)
        dense.compute(3, dense_unit)
        for i in (2, 3):
            loads[4 * layer + i].wait()
        expert.compute(0, expert_unit)
        expert.arrive(1)
        expert.compute(1, expert_unit)
        expert.arrive(2)
        expert.compute(2, expert_unit)
        expert.scatter_near()
        expert.arrive(3)
        expert.compute(3, expert_unit)
        expert.scatter_far()
        dense.scatter_near()
        expert.scatter_last()
        dense.scatter_far()
        block = jnp.concatenate([expert.total(h) for h in (0, 1)], axis=0).astype(BF)
        message = iota((slots, 2 * rows), 0)
        unpack = packed_row(message, place, per_dev, cap) == iota((slots, 2 * rows), 1)
        messages = (
            dot(jnp.where(unpack, 1.0, 0.0).astype(BF), block)
            .astype(BF)
            .reshape(n_ex, PAD, width)
        )
        back.out[...] = messages
        back.into[0] = messages[0]
        back.start()
        dense.scatter_last()
        summed = jnp.concatenate([dense.total(h) for h in (0, 1)], axis=0)
        back.arrived()
        found = dot(spot.astype(BF), back.into[...].reshape(slots, width))
        result = (x + summed + gate * found).astype(BF)
        x = result.astype(F32)
    out[...] = result
    for thing in drains:
        thing.drain()


def ring_scratch(rows, width):
    block = lambda *lead: pltpu.VMEM((*lead, rows, width), BF)
    return [
        block(4, 2, 2),
        block(4, 2),
        block(3, 2),
        block(4, 2),
        block(3, 2),
        pltpu.SemaphoreType.DMA((12,)),
        pltpu.SemaphoreType.DMA((12,)),
        pltpu.SemaphoreType.DMA((16,)),
        pltpu.SemaphoreType.DMA((16,)),
    ]


def exchange_scratch(n_ex, width):
    one = pltpu.VMEM((n_ex, PAD, width), BF)
    sem = pltpu.SemaphoreType.DMA((n_ex,))
    return [one, one, sem, sem]


def body(n_dp, n_ex, *args):
    tokens, route_a, route_b, gain_a, gain_b, router_a, router_b = args[:7]
    dense_in_a, dense_out_a, dense_in_b, dense_out_b = args[7:11]
    expert_in_a, expert_out_a, expert_in_b, expert_out_b = args[11:15]
    weights = (
        dense_in_a,
        dense_out_a,
        expert_in_a,
        expert_out_a,
        dense_in_b,
        dense_out_b,
        expert_in_b,
        expert_out_b,
    )
    tok, width = tokens.shape
    scratch = [pltpu.VMEM(w.shape, BF) for w in weights]
    scratch.append(pltpu.SemaphoreType.DMA((8,)))
    per_half = []
    layers = []
    for router in (router_a, router_b):
        experts = router.shape[1]
        cap = (5 * tok + 4 * experts - 1) // (4 * experts)
        rows = experts * cap // 2
        per_half.append(rows)
        layers += ring_scratch(tok // 2, width) + ring_scratch(rows, width)
        layers += exchange_scratch(n_ex, width) * 2
    scratch.append(pltpu.VMEM((4, 2, tok // 2, width), F32))
    scratch.append(pltpu.VMEM((4, 2, max(per_half), width), F32))
    scratch += layers
    vmem = pl.BlockSpec(memory_space=pltpu.VMEM)
    return pl.pallas_call(
        functools.partial(kernel, n_dp, n_ex),
        out_shape=jax.ShapeDtypeStruct((tok, width), BF),
        in_specs=[vmem] * 7 + [pl.BlockSpec(memory_space=pl.ANY)] * 8,
        out_specs=vmem,
        scratch_shapes=scratch,
        compiler_params=pltpu.CompilerParams(
            collective_id=0, has_side_effects=True, vmem_limit_bytes=67043328
        ),
    )(
        tokens,
        route_a,
        route_b,
        gain_a.reshape(1, width),
        gain_b.reshape(1, width),
        router_a,
        router_b,
        *weights,
    )


def solution(mesh):
    in_specs = (
        P(("dp", "expert"), None),
        P(("dp", "expert"), None),
        P(("dp", "expert"), None),
        P(),
        P(),
        P(),
        P(),
        P(None, "dp"),
        P("dp", None),
        P(None, "dp"),
        P("dp", None),
        P("expert", None, "dp"),
        P("expert", "dp", None),
        P("expert", None, "dp"),
        P("expert", "dp", None),
    )
    out_specs = P(("dp", "expert"), None)
    return jax.shard_map(
        functools.partial(body, mesh.shape["dp"], mesh.shape["expert"]),
        mesh=mesh,
        in_specs=in_specs,
        out_specs=out_specs,
        check_vma=False,
    )
```

```python
import functools

import jax
import jax.numpy as jnp
from jax import lax
from jax.experimental import pallas as pl
from jax.experimental.pallas import tpu as pltpu
from jax.sharding import PartitionSpec as P

MESH = pl.DeviceIdType.MESH
BF = jnp.bfloat16
F32 = jnp.float32
LANES = 128


def dot(a, b):
    return jnp.dot(a, b, preferred_element_type=F32)


def ffn(rows, w_in, w_out):
    return dot(jax.nn.gelu(dot(rows, w_in), approximate=True).astype(BF), w_out)


class Place:
    def __init__(self, n_dp, n_ex):
        self.n_ex = n_ex
        chips = n_dp // 2
        self.d = lax.axis_index("dp")
        self.e = lax.axis_index("expert")
        x, c = self.d // 2, self.d % 2
        right = (lax.rem(x + 1, chips) * 2 + c, self.e)
        left = (lax.rem(x + chips - 1, chips) * 2 + c, self.e)
        self.along = (right, left)
        self.partner = (x * 2 + 1 - c, self.e)

    def ahead(self, o):
        return (self.d, lax.rem(self.e + o, self.n_ex))

    def behind(self, o):
        return (self.d, lax.rem(self.e + self.n_ex - o, self.n_ex))


class Ring:
    def __init__(self, name, place, blocks, partial, kept, sums, landed, sems):
        self.name = name
        self.p = place
        self.g = blocks
        self.y1 = partial
        self.y0 = kept
        self.s = sums
        self.z = landed[0]
        self.f = landed[1]
        self.link_send, self.link_recv, self.core_send, self.core_recv = sems
        self.started = []

    def copy(self, src, dst, kind, slot, to):
        send, recv = (self.link_send, self.link_recv) if kind else (self.core_send, self.core_recv)
        return pltpu.make_async_remote_copy(
            src_ref=src,
            dst_ref=dst,
            send_sem=send.at[slot],
            recv_sem=recv.at[slot],
            device_id=to,
            device_id_type=MESH,
        )

    def start(self, make):
        made = make
        made.start()
        self.started.append(made)

    def gather_copy(self, u, h):
        if u == 1:
            return self.copy(self.g.at[0, h, 0], self.g.at[1, h, 0], 1, h, self.p.along[h])
        if u == 2:
            return self.copy(self.g.at[0, h, 0], self.g.at[2, h, 0], 1, 2 + h, self.p.along[1 - h])
        return self.copy(self.g.at[1, h, 0], self.g.at[3, h, 0], 1, 4 + h, self.p.along[h])

    def core_copy(self, u, h):
        return self.copy(self.g.at[u, h, 0], self.g.at[u, h, 1], 0, 2 * u + h, self.p.partner)

    def gather_start(self):
        for u in (1, 2):
            for h in (0, 1):
                self.start(self.gather_copy(u, h))
        for h in (0, 1):
            self.start(self.core_copy(0, h))

    def arrive(self, u):
        for h in (0, 1):
            with jax.named_scope(f"w_{self.name}_gather{u}{h}"):
                self.gather_copy(u, h).wait_recv()
            if u == 1:
                self.start(self.gather_copy(3, h))
            self.start(self.core_copy(u, h))

    def compute(self, u, fn):
        with jax.named_scope(f"w_{self.name}_core{u}"):
            for h in (0, 1):
                self.core_copy(u, h).wait_recv()
        with jax.named_scope(f"c_{self.name}{u}"):
            fn(u)
        for h in (0, 1):
            self.start(self.sum_copy(u, h))

    def sum_copy(self, u, h):
        return self.copy(self.y1.at[u, h], self.z.at[u, h], 0, 8 + 2 * u + h, self.p.partner)

    def core_sum(self, u, h):
        with jax.named_scope(f"w_{self.name}_sum{u}{h}"):
            self.sum_copy(u, h).wait_recv()
        return self.y0[u, h] + self.z[u, h].astype(F32)

    def scatter_copy(self, u, h):
        to = self.p.along[1 - h] if u == 1 else self.p.along[h]
        slot = {1: 0, 3: 1, 2: 2}[u]
        return self.copy(self.s.at[slot, h], self.f.at[slot, h], 1, 6 + 2 * slot + h, to)

    def scatter_near(self):
        for h in (0, 1):
            self.s[0, h] = self.core_sum(1, h).astype(BF)
            self.start(self.scatter_copy(1, h))

    def scatter_far(self):
        for h in (0, 1):
            self.s[1, h] = self.core_sum(3, h).astype(BF)
            self.start(self.scatter_copy(3, h))

    def scatter_last(self):
        for h in (0, 1):
            mine = self.core_sum(2, h)
            with jax.named_scope(f"w_{self.name}_scatfar{h}"):
                self.scatter_copy(3, h).wait_recv()
            self.s[2, h] = (mine + self.f[1, h].astype(F32)).astype(BF)
            self.start(self.scatter_copy(2, h))

    def total(self, h):
        mine = self.core_sum(0, h)
        with jax.named_scope(f"w_{self.name}_scatnear{h}"):
            self.scatter_copy(1, h).wait_recv()
        mine = mine + self.f[0, h].astype(F32)
        with jax.named_scope(f"w_{self.name}_scatlast{h}"):
            self.scatter_copy(2, h).wait_recv()
        return mine + self.f[2, h].astype(F32)

    def drain(self):
        for made in self.started:
            made.wait_send()


class Exchange:
    def __init__(self, place, rows, stage, refs, forward):
        self.p, self.rows, self.forward = place, rows, forward
        self.out, self.into, self.send, self.recv = refs
        self.stage = stage.at[pl.ds(0, place.n_ex * rows)]

    def copy(self, o):
        message = pl.ds(o * self.rows, self.rows)
        return pltpu.make_async_remote_copy(
            src_ref=self.out.at[message],
            dst_ref=self.into.at[message],
            send_sem=self.send.at[o],
            recv_sem=self.recv.at[o],
            device_id=self.p.ahead(o) if self.forward else self.p.behind(o),
            device_id_type=MESH,
        )

    def each(self, act):
        def one(o, carry):
            act(self.copy(o))
            return carry

        lax.fori_loop(1, self.p.n_ex, one, 0)

    def start(self, value):
        for j in range(value.shape[1] // LANES):
            self.stage[:, j, :] = value[:, j * LANES : (j + 1) * LANES]
        tiles = self.stage[...].astype(BF)
        self.out[...] = tiles
        self.into[pl.ds(0, self.rows)] = tiles[: self.rows]
        self.each(lambda copy: copy.start())

    def arrived(self):
        with jax.named_scope(f"w_a2a{int(self.forward)}"):
            self.each(lambda copy: copy.wait_recv())
        self.stage[...] = self.into[...].astype(F32)
        columns = [self.stage[:, j, :] for j in range(self.into.shape[1])]
        return jnp.concatenate(columns, axis=1).astype(BF)

    def drain(self):
        self.each(lambda copy: copy.wait_send())


def norm_rows(xf, gain):
    mean = jnp.mean(xf, axis=-1, keepdims=True)
    var = jnp.mean((xf - mean) ** 2, axis=-1, keepdims=True)
    return ((xf - mean) / jnp.sqrt(var + 1e-05) * gain).astype(BF)


def iota(shape, dim):
    return lax.broadcasted_iota(jnp.int32, shape, dim)


def routing(ids, place, experts, cap):
    tok = ids.shape[1]
    per_dev = experts // place.n_ex
    onehot = (iota((experts, tok), 0) == ids).astype(F32)
    earlier = (iota((tok, tok), 0) < iota((tok, tok), 1)).astype(F32)
    before = dot(onehot.astype(BF), earlier.astype(BF))
    rank = jnp.sum(before * onehot, axis=0, keepdims=True)
    kept = rank < cap
    owner, inner = ids // per_dev, ids % per_dev
    offset = lax.rem(owner - place.e + place.n_ex, place.n_ex)
    row = ((offset * per_dev + inner) * cap).astype(F32) + rank
    rows = place.n_ex * per_dev * cap
    spot = jnp.where(kept & (iota((rows, tok), 0).astype(F32) == row), 1.0, 0.0)
    return onehot, kept, spot


def by_expert(shape, dim, place, per_dev, cap):
    message, packed = iota(shape, 1 - dim), iota(shape, dim)
    source, inner = message // (per_dev * cap), message % (per_dev * cap)
    which, rank = inner // cap, inner % cap
    row = (which * place.n_ex + source) * cap + rank
    return jnp.where(packed == row, 1.0, 0.0).astype(BF)


def kernel(
    n_dp,
    n_ex,
    *refs,
):
    (tokens, route_a, route_b, gain_a, gain_b, router_a, router_b) = refs[:7]
    weights = refs[7:15]
    out = refs[15]
    local = refs[16:24]
    weight_sem = refs[24]
    scratch = refs[25:]
    place = Place(n_dp, n_ex)
    loads = [
        pltpu.make_async_copy(weights[i], local[i], weight_sem.at[i]) for i in range(8)
    ]
    barrier = pltpu.get_barrier_semaphore()

    def greet(o, carry):
        pl.semaphore_signal(barrier, inc=1, device_id=place.ahead(o), device_id_type=MESH)
        return carry

    for to in (*place.along, place.partner):
        pl.semaphore_signal(barrier, inc=1, device_id=to, device_id_type=MESH)
    lax.fori_loop(1, n_ex, greet, 0)
    for i in (0, 1, 4, 5, 2, 3, 6, 7):
        loads[i].start()

    kept_dense, kept_expert, stage = scratch[:3]
    scratch = scratch[3:]
    per_layer = len(scratch) // 2
    drains = []
    x = tokens[...].astype(F32)
    for layer in range(2):
        s = scratch[layer * per_layer : (layer + 1) * per_layer]
        dense = Ring("d", place, s[0], s[1], kept_dense, s[2], s[3:5], s[5:9])
        s = s[9:]
        rows = s[0].shape[3]
        y0 = kept_expert.at[:, :, pl.ds(0, rows)]
        expert = Ring("e", place, s[0], s[1], y0, s[2], s[3:5], s[5:9])
        s = s[9:]
        router = (router_a, router_b)[layer][...]
        experts = router.shape[0]
        tok, width = tokens.shape
        per_dev = experts // n_ex
        cap = (5 * tok + 4 * experts - 1) // (4 * experts)
        go = Exchange(place, per_dev * cap, stage, s[0:4], True)
        back = Exchange(place, per_dev * cap, stage, s[4:8], False)
        drains += [dense, expert, go, back]
        ids = (route_a, route_b)[layer][...]
        d_in, d_out = local[4 * layer], local[4 * layer + 1]
        e_in, e_out = local[4 * layer + 2], local[4 * layer + 3]
        half = tok // 2

        normed = norm_rows(x, (gain_a, gain_b)[layer][...])
        for h in (0, 1):
            dense.g[0, h, 0] = normed[h * half : (h + 1) * half]
        onehot, kept, spot = routing(ids, place, experts, cap)
        if layer == 0:
            with jax.named_scope("w_barrier"):
                pl.semaphore_wait(barrier, n_ex - 1 + 3)
        dense.gather_start()
        go.start(dot(spot.astype(BF), normed))
        logits = lax.dot_general(
            router, normed, (((1,), (1,)), ((), ())), preferred_element_type=F32
        )
        picked = jnp.sum(logits * onehot, axis=0, keepdims=True)
        gate = jax.nn.sigmoid(picked) * kept.astype(F32)
        gate = jnp.broadcast_to(gate, (tok, tok)).T[:, :1]

        def dense_unit(u):
            y = ffn(dense.g[u].reshape(4 * half, width), d_in[...], d_out[...])
            y = y.reshape(2, 2, half, width)
            dense.y1[u] = y[:, 1].astype(BF)
            dense.y0[u] = y[:, 0]

        def expert_unit(u):
            if per_dev == 1:
                y = ffn(expert.g[u].reshape(4 * rows, width), e_in[0], e_out[0])
                y = y.reshape(2, 2, rows, width)
                expert.y1[u] = y[:, 1].astype(BF)
                expert.y0[u] = y[:, 0]
            else:
                for h in (0, 1):
                    y = ffn(expert.g[u, h].reshape(2 * rows, width), e_in[h], e_out[h])
                    y = y.reshape(2, rows, width)
                    expert.y1[u, h] = y[1].astype(BF)
                    expert.y0[u, h] = y[0]

        for i in (0, 1):
            loads[4 * layer + i].wait()
        dense.compute(0, dense_unit)
        dense.arrive(1)
        dense.compute(1, dense_unit)
        dense.arrive(2)

        block = go.arrived()
        slots = (2 * rows, 2 * rows)
        if per_dev > 1:
            block = dot(by_expert(slots, 0, place, per_dev, cap), block).astype(BF)
        for h in (0, 1):
            expert.g[0, h, 0] = block[h * rows : (h + 1) * rows]
        expert.gather_start()
        dense.compute(2, dense_unit)
        dense.arrive(3)
        dense.compute(3, dense_unit)
        for i in (2, 3):
            loads[4 * layer + i].wait()
        expert.compute(0, expert_unit)
        expert.arrive(1)
        expert.compute(1, expert_unit)
        expert.arrive(2)
        expert.compute(2, expert_unit)
        expert.scatter_near()
        expert.arrive(3)
        expert.compute(3, expert_unit)
        expert.scatter_far()
        dense.scatter_near()
        expert.scatter_last()
        dense.scatter_far()
        block = jnp.concatenate([expert.total(h) for h in (0, 1)], axis=0)
        if per_dev > 1:
            block = dot(by_expert(slots, 1, place, per_dev, cap), block.astype(BF))
        back.start(block)
        dense.scatter_last()
        summed = jnp.concatenate([dense.total(h) for h in (0, 1)], axis=0)
        found = lax.dot_general(
            spot.astype(BF), back.arrived(), (((0,), (0,)), ((), ())), preferred_element_type=F32
        )
        result = (x + summed + gate * found).astype(BF)
        x = result.astype(F32)
    out[...] = result
    with jax.named_scope("w_drain"):
        for thing in drains:
            thing.drain()


def ring_scratch(rows, width):
    block = lambda *lead: pltpu.VMEM((*lead, rows, width), BF)
    return [
        block(4, 2, 2),
        block(4, 2),
        block(3, 2),
        block(4, 2),
        block(3, 2),
        pltpu.SemaphoreType.DMA((12,)),
        pltpu.SemaphoreType.DMA((12,)),
        pltpu.SemaphoreType.DMA((16,)),
        pltpu.SemaphoreType.DMA((16,)),
    ]


def exchange_scratch(n_ex, slots, width):
    one = pltpu.VMEM((slots, width // LANES, LANES), BF)
    sem = pltpu.SemaphoreType.DMA((n_ex,))
    return [one, one, sem, sem]


def body(n_dp, n_ex, *args):
    tokens, route_a, route_b, gain_a, gain_b, router_a, router_b = args[:7]
    dense_in_a, dense_out_a, dense_in_b, dense_out_b = args[7:11]
    expert_in_a, expert_out_a, expert_in_b, expert_out_b = args[11:15]
    weights = (
        dense_in_a,
        dense_out_a,
        expert_in_a,
        expert_out_a,
        dense_in_b,
        dense_out_b,
        expert_in_b,
        expert_out_b,
    )
    tok, width = tokens.shape
    scratch = [pltpu.VMEM(w.shape, BF) for w in weights]
    scratch.append(pltpu.SemaphoreType.DMA((8,)))
    per_half = []
    layers = []
    for router in (router_a, router_b):
        experts = router.shape[1]
        cap = (5 * tok + 4 * experts - 1) // (4 * experts)
        rows = experts * cap // 2
        per_half.append(rows)
        layers += ring_scratch(tok // 2, width) + ring_scratch(rows, width)
        layers += exchange_scratch(n_ex, 2 * rows, width) * 2
    scratch.append(pltpu.VMEM((4, 2, tok // 2, width), F32))
    scratch.append(pltpu.VMEM((4, 2, max(per_half), width), F32))
    scratch.append(pltpu.VMEM((2 * max(per_half), width // LANES, LANES), F32))
    scratch += layers
    vmem = pl.BlockSpec(memory_space=pltpu.VMEM)
    return pl.pallas_call(
        functools.partial(kernel, n_dp, n_ex),
        out_shape=jax.ShapeDtypeStruct((tok, width), BF),
        in_specs=[vmem] * 7 + [pl.BlockSpec(memory_space=pl.ANY)] * 8,
        out_specs=vmem,
        scratch_shapes=scratch,
        compiler_params=pltpu.CompilerParams(
            collective_id=0, has_side_effects=True, vmem_limit_bytes=67043328
        ),
    )(
        tokens,
        route_a.reshape(1, tok),
        route_b.reshape(1, tok),
        gain_a.reshape(1, width),
        gain_b.reshape(1, width),
        router_a.T,
        router_b.T,
        *weights,
    )


def solution(mesh):
    in_specs = (
        P(("dp", "expert"), None),
        P(("dp", "expert"), None),
        P(("dp", "expert"), None),
        P(),
        P(),
        P(),
        P(),
        P(None, "dp"),
        P("dp", None),
        P(None, "dp"),
        P("dp", None),
        P("expert", None, "dp"),
        P("expert", "dp", None),
        P("expert", None, "dp"),
        P("expert", "dp", None),
    )
    out_specs = P(("dp", "expert"), None)
    return jax.shard_map(
        functools.partial(body, mesh.shape["dp"], mesh.shape["expert"]),
        mesh=mesh,
        in_specs=in_specs,
        out_specs=out_specs,
        check_vma=False,
    )
```
